256 devices in a mesh: group: 4 (over y), dom: 64 (over x, z, core).
Axes of the slice: x: 4, y: 4, z: 8, core: 2. Of those that a mesh axis runs over, the one named last changes fastest.
Arguments:
- features: bfloat16 [2, 65536, 1024], P(None, ('group', 'dom')), may hold values from -6 to 6
- adjacency: bfloat16 [65536, 256], P(('group', 'dom')), may hold values from -0.375 to 0.375
- tile_mask: int32 [512, 2], P(('group', 'dom')), may hold values 0 or 1
- boundary_adj: bfloat16 [65536, 1024], P(('group', 'dom')), may hold values from -0.1875 to 0.1875
- boundary_blocks: int32 [4, 64, 4, 2], P('group'), may hold values from -1 to 1
- hub_adj: bfloat16 [256, 65536], P(None, ('group', 'dom')), may hold values from -0.09375 to 0.09375
- hub_offsets: int32 [4, 256], P('group', 'dom'), may hold values from 0 to 63
- weight: bfloat16 [1024, 1024], replicated, may hold values from -0.1875 to 0.1875
- cotangent: bfloat16 [2, 65536, 1024], P(None, ('group', 'dom')), may hold values from -24 to 24
Outputs:
- activations: bfloat16 [2, 65536, 1024], P(None, ('group', 'dom'))
- input_grad: bfloat16 [2, 65536, 1024], P(None, ('group', 'dom'))
- carried_grad: bfloat16 [65536, 1024], P(('group', 'dom'))
- weight_grad: float32 [1024, 1024], P(('group', 'dom'))
The draws below stay inside these ranges and needn't reach their ends.
Inputs may be any that keep to these rules, and one draw needn't show every extreme that they name: `boundary_blocks`: entry [g, d, o, j] names the block that cluster (g, d) requests in slot j from the cluster at dom index d + s_o (s_o as in the reference program); -1 marks an unused slot; a slot whose source lies outside the group receives zeros. `hub_offsets`: gives the row of hub h's mirror in cluster (g, h // 4) as stated in the reference program. `tile_mask`: 1 where a tile of local edges is present.
All inputs are finite; a program needn't handle non-finite values. No bound on the sum of `tile_mask` on one device may be relied on, other than what follows from the above.
Results may differ from the reference program's by a relative error of at most 0.0067.
Values may be sent and summed in bfloat16 or wider, within the bound.
No kernel may reach another device: no remote copies, remote signals or barrier semaphores. Data moves between devices by JAX's collectives and lax.ppermute only.
A program may use at most 64 MiB of HBM per device.

```python
import jax
import jax.numpy as jnp
from jax import lax

D = 1024
NODES = 256
BLK = 128
CAPB = 2
HUB_DEV = 4
ITERS = 2
NB = 2
OFFS = 4
SLOTS = 8
GROUPS = 4
DOMS = 64
ALLNODES = 65536
HUBS = 256
ALLTILES = 512


def touch_ends(drawn, rng, least, top_value):
    longest = drawn.shape.index(max(drawn.shape))
    spots = []
    for shift in (0, 1):
        where = [jax.random.randint(jax.random.fold_in(rng, axis), (), 0, length) for axis, length in enumerate(drawn.shape)]
        where[longest] = (where[longest] + shift) % drawn.shape[longest]
        spots.append(tuple(where))
    return drawn.at[spots[0]].set(least).at[spots[1]].set(top_value)


def strengthened(drawn, key, source, target, blocks, factor):
    owner, partner = [(jnp.arange(drawn.shape[dim]) // (drawn.shape[dim] // blocks)).reshape([-1 if axis == dim else 1 for axis in range(drawn.ndim)]) for dim in (source, target)]
    chosen = jax.random.permutation(key, blocks)[partner]
    strong = (owner == chosen) | (owner == (partner + blocks // 2) % blocks)
    return jnp.where(strong, factor * drawn, drawn)


def block_levels(key, dims, cuts, low, largest):
    loudness = 1.0
    for dim, blocks in cuts:
        steps = jax.random.uniform(jax.random.fold_in(jax.random.fold_in(key, 6), dim), (blocks,), jnp.float32, low / len(cuts), largest / len(cuts))
        loudness = loudness * jnp.repeat(jnp.exp(steps), dims[dim] // blocks).reshape((-1,) + (1,) * (len(dims) - 1 - dim))
    return loudness


def bell_draw(rng, shape, width, limit, split=(), kind=jnp.bfloat16):
    factor_of = block_levels(rng, shape, split, -0.22, 0.18) if split else 1.0
    entries = jax.random.normal(rng, shape, jnp.float32) * width * factor_of
    return jnp.minimum(jnp.maximum(entries, -limit), limit).astype(kind)


def bell_draw_with(own_key, dims, scale, bound, cuts, heavy, held_as=jnp.bfloat16):
    drawn = scale * jax.random.normal(own_key, dims, jnp.float32)
    if cuts:
        drawn = drawn * block_levels(own_key, dims, cuts, -0.22, 0.18)
    return jnp.clip(strengthened(drawn, jax.random.fold_in(own_key, 3), *heavy), -bound, bound).astype(held_as)


def setup_inputs(seed: int = 0) -> dict:
    seeds = jax.random.split(jax.random.key(seed), 10)
    return {
        "features": bell_draw(seeds[0], (ITERS, ALLNODES, D), 1.0, 6.0, ((1, 256),)),
        "adjacency": bell_draw(seeds[1], (ALLNODES, NODES), NODES ** -0.5, 0.375, ((0, 256),)),
        "tile_mask": touch_ends((jax.random.randint(seeds[2], (ALLTILES, NB), 0, 4) < 3).astype(jnp.int32), jax.random.fold_in(seeds[2], 1), 0, 1),
        "boundary_adj": bell_draw(seeds[3], (ALLNODES, SLOTS * BLK), (SLOTS * BLK) ** -0.5, 0.1875, ((0, 256),)),
        "boundary_blocks": touch_ends(jax.random.randint(seeds[4], (GROUPS, DOMS, OFFS, CAPB), -1, NB), jax.random.fold_in(seeds[4], 1), -1, NB - 1).astype(jnp.int32),
        "hub_adj": bell_draw_with(seeds[5], (HUBS, ALLNODES), ALLNODES ** -0.5, 0.09375, ((1, 256),), (1, 0, 256, 6.0)),
        "hub_offsets": touch_ends(jax.random.randint(seeds[6], (GROUPS, HUBS), 0, NODES // HUB_DEV), jax.random.fold_in(seeds[6], 1), 0, (NODES // HUB_DEV) - 1).astype(jnp.int32),
        "weight": bell_draw(seeds[7], (D, D), D ** -0.5, 0.1875),
        "cotangent": bell_draw_with(seeds[8], (ITERS, ALLNODES, D), 1.0, 24.0, ((1, 256),), (1, 2, 256, 6.0)),
    }


def offset_of(order):
    return (order // 2 + 1) * (1 - 2 * (order % 2))


def reference(features, adjacency, tile_mask, boundary_adj, boundary_blocks, hub_adj, hub_offsets, weight, cotangent):
    devs = GROUPS * DOMS
    spread = jnp.repeat(jnp.repeat(tile_mask.reshape(devs, NB, NB), BLK, axis=1), BLK, axis=2).astype(jnp.bfloat16)
    local_adj = adjacency.reshape(devs, NODES, NODES) * spread
    bound_adj = boundary_adj.reshape(devs, NODES, SLOTS * BLK)
    hub_cols = jnp.transpose(hub_adj.reshape(HUBS, devs, NODES), (1, 0, 2))
    stride = NODES // HUB_DEV
    hub_rows = ((jnp.arange(HUBS, dtype=jnp.int32) % HUB_DEV) * stride)[None, :] + hub_offsets
    hub_rows = hub_rows.astype(jnp.int32).reshape(devs, HUB_DEV)
    shifts = jnp.array([offset_of(o) for o in range(OFFS)], dtype=jnp.int32)
    source = jnp.arange(DOMS, dtype=jnp.int32)[:, None] + shifts[None, :]
    inside = (source >= 0) & (source < DOMS)
    source = jnp.clip(source, 0, DOMS - 1).astype(jnp.int32)
    live = (boundary_blocks >= 0) & inside[None, :, :, None]
    block = jnp.clip(boundary_blocks, 0, NB - 1).astype(jnp.int32)
    groups = jnp.arange(GROUPS, dtype=jnp.int32)[:, None]
    first = features[0].reshape(GROUPS, DOMS, NB, BLK, D)
    pieces = []
    for o in range(OFFS):
        for j in range(CAPB):
            got = first[groups, source[None, :, o], block[:, :, o, j]]
            pieces.append(jnp.where(live[:, :, o, j][:, :, None, None], got, jnp.zeros_like(got)))
    received = jnp.stack(pieces, axis=2).reshape(devs, SLOTS * BLK, D)
    scale = (ITERS * NODES * devs) ** -0.5
    acts, grads = [], []
    weight_total = jnp.zeros((D, D), jnp.float32)
    carried = jnp.zeros((GROUPS, DOMS, NB, BLK, D), jnp.float32)
    for step in range(ITERS):
        feats = features[step].reshape(devs, NODES, D)
        hub_sum = jnp.dot(hub_adj, features[step], preferred_element_type=jnp.float32)
        hub_blocks = jnp.broadcast_to(hub_sum.reshape(1, DOMS, HUB_DEV, D), (GROUPS, DOMS, HUB_DEV, D)).reshape(devs, HUB_DEV, D)
        cot = cotangent[step].reshape(devs, NODES, D)

        def forward(items):
            adj, bnd, feat, recv, rows, hubs, grad_out = items
            total = jnp.dot(adj, feat, preferred_element_type=jnp.float32) + jnp.dot(bnd, recv, preferred_element_type=jnp.float32)
            total = total.at[rows].add(hubs)
            agg = total.astype(jnp.bfloat16)
            pre = jnp.dot(agg, weight.T, preferred_element_type=jnp.float32)
            act = jax.nn.silu(pre).astype(jnp.bfloat16)
            sig = jax.nn.sigmoid(pre)
            gpre = (grad_out.astype(jnp.float32) * sig * (1.0 + pre * (1.0 - sig))).astype(jnp.bfloat16)
            dagg = jnp.dot(gpre, weight, preferred_element_type=jnp.float32).astype(jnp.bfloat16)
            local = jnp.dot(adj.T, dagg, preferred_element_type=jnp.float32)
            bgrad = jnp.dot(bnd.T, dagg, preferred_element_type=jnp.float32).astype(jnp.bfloat16)
            mirror = dagg[rows]
            return agg, act, gpre, local, bgrad, mirror

        agg, act, gpre, local, bgrad, mirror = lax.map(forward, (local_adj, bound_adj, feats, received, hub_rows, hub_blocks, cot))
        hub_grad = jnp.sum(mirror.reshape(GROUPS, HUBS, D).astype(jnp.float32), axis=0)

        def hub_back(cols):
            return jnp.dot(cols.astype(jnp.float32).T, hub_grad, precision=lax.Precision.HIGHEST)

        hub_term = lax.map(hub_back, hub_cols)
        back = jnp.zeros((GROUPS, DOMS, NB, BLK, D), jnp.float32)
        slots = bgrad.reshape(GROUPS, DOMS, OFFS, CAPB, BLK, D)
        for o in range(OFFS):
            for j in range(CAPB):
                vals = jnp.where(live[:, :, o, j][:, :, None, None], slots[:, :, o, j].astype(jnp.float32), jnp.zeros((GROUPS, DOMS, BLK, D), jnp.float32))
                back = back.at[groups, source[None, :, o], block[:, :, o, j]].add(vals)
        grads.append((local + hub_term + carried.reshape(devs, NODES, D)).astype(jnp.bfloat16).reshape(ALLNODES, D))
        acts.append(act.reshape(ALLNODES, D))
        carried = back
        weight_total = weight_total + jnp.dot(gpre.reshape(ALLNODES, D).T, agg.reshape(ALLNODES, D), preferred_element_type=jnp.float32)
    return (jnp.stack(acts), jnp.stack(grads), carried.reshape(ALLNODES, D).astype(jnp.bfloat16), weight_total * scale)
```

```python
import jax
import jax.numpy as jnp
from jax import lax
from jax.experimental import pallas as pl
from jax.experimental.pallas import tpu as pltpu
from jax.sharding import PartitionSpec as P


BLK = 128
HUB_DEV = 4
CORES = 2
XS = 4
ZS = 8
GROUPS = 4
F32 = jnp.float32
BF16 = jnp.bfloat16


def dom_index(x, z, c):
    return (x * ZS + z) * CORES + c


def dom_pairs(target):
    pairs = []
    for x in range(XS):
        for z in range(ZS):
            for c in range(CORES):
                pairs.append((dom_index(x, z, c), target(x, z, c)))
    return pairs


def swap(v):
    return lax.ppermute(v, "dom", dom_pairs(lambda x, z, c: dom_index(x, z, 1 - c)))


def along_x(v, k):
    return lax.ppermute(v, "dom", dom_pairs(lambda x, z, c: dom_index((x + k) % XS, z, c)))


def across_z(v, bit):
    return lax.ppermute(v, "dom", dom_pairs(lambda x, z, c: dom_index(x, z ^ bit, c)))


def along_y(v, k):
    return lax.ppermute(v, "group", [(y, (y + k) % GROUPS) for y in range(GROUPS)])


def chip_step(v, even_by):
    count = XS * ZS * CORES
    pairs = []
    for d in range(count):
        to = d + (even_by if d % 2 == 0 else -even_by)
        if 0 <= to < count:
            pairs.append((d, to))
    return lax.ppermute(v, "dom", pairs)


def first_step(v):
    return chip_step(v, -2)


def second_step(v):
    return chip_step(v, 2)


def dot(a, b):
    return lax.dot_general(a, b, (((1,), (0,)), ((), ())), preferred_element_type=F32)


def dot_tn(a, b):
    return lax.dot_general(a, b, (((0,), (0,)), ((), ())), preferred_element_type=F32)


def dot_nt(a, b):
    return lax.dot_general(a, b, (((1,), (1,)), ((), ())), preferred_element_type=F32)


def relative_rows(shape, with_group, here, y):
    c = here & 1
    z = (here >> 1) & (ZS - 1)
    x = here >> 4
    r = lax.broadcasted_iota(jnp.int32, shape, 0)
    low = r & 3
    zz = z ^ (((r >> 4) & 1) + (((r >> 3) & 1) << 1) + (((r >> 2) & 1) << 2))
    xx = (x + (r >> 5)) & 3
    if with_group:
        yy = (y + (r >> 7)) & 3
        return (yy << 8) + (xx << 6) + (zz << 3) + ((c ^ (r >> 9)) << 2) + low
    return (xx << 6) + (zz << 3) + ((c ^ (r >> 7)) << 2) + low


VM = pl.BlockSpec(memory_space=pltpu.VMEM)
SM = pl.BlockSpec(memory_space=pltpu.SMEM)
ANY = pl.BlockSpec(memory_space=pl.ANY)


def call(body, specs, outs, flops, *args):
    shapes = [jax.ShapeDtypeStruct(s, d) for s, d in outs]
    moved = sum(a.size * a.dtype.itemsize for a in args) + sum(s.size * s.dtype.itemsize for s in shapes)
    kernel = pl.pallas_call(
        body,
        out_shape=shapes,
        in_specs=specs,
        out_specs=[VM] * len(shapes),
        cost_estimate=pl.CostEstimate(flops=flops, bytes_accessed=moved, transcendentals=0),
        compiler_params=pltpu.CompilerParams(vmem_limit_bytes=16 * 1024 * 1024),
    )
    return kernel(*args)


def hub_kernel(hub_ref, f_ref, rel_ref, pay_ref, f0_ref, mine_ref):
    target = relative_rows((256, 256), False, lax.axis_index("dom"), 0)
    col = lax.broadcasted_iota(jnp.int32, (256, 256), 1)
    perm = jnp.where(target == col, 1.0, 0.0).astype(BF16)
    ordered = dot(perm, hub_ref[...])
    rel = ordered.astype(BF16)
    rel_ref[...] = jnp.transpose(ordered).astype(BF16)
    for t in range(2):
        for n in range(0, 1024, 256):
            p = dot(rel, f_ref[t, :, n : n + 256])
            mine_ref[:, t * 1024 + n : t * 1024 + n + 256] = p[:128]
            pay_ref[t * 128 : t * 128 + 128, n : n + 256] = p[128:].astype(BF16)
    pay_ref[256:512, :] = f_ref[0]
    f0_ref[...] = f_ref[0]


def table_kernel(asked, present, b_ref, a_ref, roles_ref, roles_t_ref, local_ref, local_t_ref):
    c = lax.axis_index("dom") & 1
    for r in range(4):
        for b in range(2):
            total = None
            for o in (r, r ^ 1):
                for j in range(2):
                    s = 2 * o + j
                    gate = jnp.where(((r ^ c) == o) & (asked[s] == b), 1.0, 0.0)
                    term = b_ref[:, s * BLK : s * BLK + BLK].astype(F32) * gate
                    total = term if total is None else total + term
            at = (2 * r + b) * BLK
            roles_ref[:, at : at + BLK] = total.astype(BF16)
            roles_t_ref[at : at + BLK, :] = jnp.transpose(total).astype(BF16)
    for i in range(2):
        for j in range(2):
            gate = present[i, j].astype(F32)
            tile = a_ref[i * BLK : i * BLK + BLK, j * BLK : j * BLK + BLK].astype(F32) * gate
            local_ref[i * BLK : i * BLK + BLK, j * BLK : j * BLK + BLK] = tile.astype(BF16)
            local_t_ref[j * BLK : j * BLK + BLK, i * BLK : i * BLK + BLK] = jnp.transpose(tile).astype(BF16)


def open_kernel(got_ref, mine_ref, keep_ref, one_ref, two_ref, three_ref):
    for t in range(2):
        lanes = slice(t * 1024, t * 1024 + 1024)
        part = mine_ref[:, lanes] + got_ref[t * 128 : t * 128 + 128, :].astype(F32)
        keep_ref[:, lanes] = part[:32]
        one_ref[:, lanes] = part[32:64].astype(BF16)
        two_ref[:, lanes] = part[64:96].astype(BF16)
        three_ref[:, lanes] = part[96:].astype(BF16)


def total_kernel(after, roles, local, f_ref, pair_ref, far_ref, first_ref, second_ref, out_ref):
    for n in range(0, 1024, 256):
        lanes = slice(n, n + 256)
        bound = (
            dot(roles[:, :256], pair_ref[256:512, lanes])
            + dot(roles[:, 256:512], far_ref[:, lanes])
            + dot(roles[:, 512:768], first_ref[:, lanes])
            + dot(roles[:, 768:], second_ref[:, lanes])
        )
        for t in range(2):
            out_ref[t * 256 : t * 256 + 256, lanes] = bound + dot(local[...], f_ref[t, :, lanes])


def agg_kernel(offs, total_ref, own_ref, g1_ref, g2_ref, g3_ref, agg_ref):
    hubs = own_ref[...] + (g1_ref[...].astype(F32) + g2_ref[...].astype(F32) + g3_ref[...].astype(F32))
    ids = lax.broadcasted_iota(jnp.int32, (64, 1024), 0)
    for t in range(2):
        for i in range(HUB_DEV):
            at = t * 256 + i * 64
            extra = jnp.where(ids == offs[0, i], hubs[i : i + 1, t * 1024 : t * 1024 + 1024], 0.0)
            agg_ref[at : at + 64, :] = (total_ref[at : at + 64, :] + extra).astype(BF16)


def send_kernel(offs, roles_t, dagg_ref, mirror_ref, first_ref):
    cols = lax.broadcasted_iota(jnp.int32, (8, 256), 1)
    rows = lax.broadcasted_iota(jnp.int32, (8, 256), 0)
    where = jnp.where(
        rows == 0, offs[0, 0], jnp.where(rows == 1, offs[0, 1], jnp.where(rows == 2, offs[0, 2], offs[0, 3]))
    )
    pick = jnp.where((cols == rows * 64 + where) & (rows < HUB_DEV), 1.0, 0.0).astype(BF16)
    for t in range(2):
        d = dagg_ref[t * 256 : t * 256 + 256, :]
        mirror_ref[:, t * 1024 : t * 1024 + 1024] = dot(pick, d)[:HUB_DEV].astype(BF16)
        first_ref[t * 256 : t * 256 + 256, :] = dot(roles_t[768:, :], d).astype(BF16)


def pair_kernel(roles_t, dagg_ref, out_ref):
    for r in range(2):
        for t in range(2):
            at = (2 * r + t) * 256
            out_ref[at : at + 256, :] = dot(
                roles_t[r * 256 : r * 256 + 256, :], dagg_ref[t * 256 : t * 256 + 256, :]
            ).astype(BF16)


def through_kernel(roles_t, dagg_ref, got_ref, out_ref):
    for t in range(2):
        rows = slice(t * 256, t * 256 + 256)
        mine = dot(roles_t[512:768, :], dagg_ref[rows, :])
        out_ref[rows, :] = (mine + got_ref[512 + t * 256 : 768 + t * 256, :].astype(F32)).astype(BF16)


def base_kernel(local_t, dagg_ref, pair_ref, first_ref, second_ref, base_ref, carried_ref):
    base_ref[:256, :] = dot(local_t[...], dagg_ref[:256, :])
    returned = pair_ref[:512, :].astype(F32) + first_ref[...].astype(F32) + second_ref[...].astype(F32)
    base_ref[256:, :] = dot(local_t[...], dagg_ref[256:, :]) + returned[:256]
    carried_ref[...] = returned[256:].astype(BF16)


def grad_kernel(base_ref, rel_t, own_ref, got_ref, out_ref):
    for t in range(2):
        lanes = slice(t * 1024, t * 1024 + 1024)
        hub = dot(rel_t[:, :128], own_ref[:, lanes]) + dot(rel_t[:, 128:], got_ref[:, lanes])
        out_ref[t] = (base_ref[t * 256 : t * 256 + 256, :] + hub).astype(BF16)


def join_kernel(own_ref, one_ref, two_ref, three_ref, out_ref):
    out_ref[:32, :] = own_ref[...]
    out_ref[32:64, :] = one_ref[...]
    out_ref[64:96, :] = two_ref[...]
    out_ref[96:, :] = three_ref[...]


def per_device(
    features,
    adjacency,
    tile_mask,
    boundary_adj,
    boundary_blocks,
    hub_adj,
    hub_offsets,
    weight,
    cotangent,
):
    steps, nodes, width = features.shape
    here = lax.axis_index("dom")
    y = lax.axis_index("group")
    both = steps * nodes
    mm = 2 * nodes * nodes * width

    rel_t, payload, first, mine = call(
        hub_kernel,
        [VM, VM],
        [((256, 256), BF16), ((512, width), BF16), ((nodes, width), BF16), ((128, 2 * width), F32)],
        2 * mm,
        hub_adj,
        features,
    )
    from_pair = swap(payload)
    from_first = first_step(first)
    from_second = second_step(first)

    asked = lax.dynamic_index_in_dim(boundary_blocks[0], here, 0, keepdims=False).reshape(8)
    roles, roles_t, local, local_t = call(
        table_kernel,
        [SM, SM, VM, VM],
        [((nodes, width), BF16), ((width, nodes), BF16), ((nodes, nodes), BF16), ((nodes, nodes), BF16)],
        mm,
        asked,
        tile_mask,
        boundary_adj,
        adjacency,
    )

    part, *sends = call(
        open_kernel,
        [VM, VM],
        [((32, 2 * width), F32)] + [((32, 2 * width), BF16)] * 3,
        mm,
        from_pair,
        mine,
    )
    gots = [along_x(sends[k - 1], k) for k in (1, 3, 2)]
    from_far = swap(from_first)
    part = part + (gots[0].astype(F32) + gots[1].astype(F32) + gots[2].astype(F32))
    marks = []
    for bit, rows in ((1, 16), (2, 8), (4, 4)):
        sent = part[rows:].astype(BF16)
        marks.append(sent)
        got = across_z(sent, bit)
        part = part[:rows] + got.astype(F32)
    sent = part.astype(BF16)
    gots = [along_y(sent, k) for k in (1, 3, 2)]

    (total,) = call(
        total_kernel,
        [ANY, VM, VM, VM, VM, VM, VM, VM],
        [((both, width), F32)],
        6 * mm,
        marks[1],
        roles,
        local,
        features,
        from_pair,
        from_far,
        from_first,
        from_second,
    )
    (agg,) = call(
        agg_kernel,
        [SM, VM, VM, VM, VM, VM],
        [((both, width), BF16)],
        mm,
        hub_offsets,
        total,
        part,
        *gots,
    )
    pre = dot_nt(agg, weight)
    sig = jax.nn.sigmoid(pre)
    act = (pre * sig).astype(BF16)
    gpre = (cotangent.reshape(both, width).astype(F32) * sig * (1.0 + pre * (1.0 - sig))).astype(BF16)

    perm = relative_rows((width, width), True, here, y) == lax.broadcasted_iota(jnp.int32, (width, width), 1)
    perm = perm.astype(BF16)
    perm = lax.optimization_barrier(perm)
    gpre_rel = lax.optimization_barrier(dot_nt(gpre, perm).astype(BF16))
    got_w = swap(dot_tn(gpre_rel[:, 512:], agg).astype(BF16))
    dagg = dot(gpre, weight).astype(BF16)

    mirror, to_first = call(
        send_kernel,
        [SM, VM, VM],
        [((HUB_DEV, 2 * width), BF16), ((both, width), BF16)],
        2 * mm,
        hub_offsets,
        roles_t,
        dagg,
    )
    gots = [along_y(mirror, k) for k in (1, 3, 2)]
    back_first = first_step(to_first)
    (to_pair,) = call(pair_kernel, [VM, VM], [((2 * both, width), BF16)], 4 * mm, roles_t, dagg)
    back_pair = swap(to_pair)
    gathered = (
        mirror.astype(F32) + (gots[0].astype(F32) + gots[1].astype(F32) + gots[2].astype(F32))
    ).astype(BF16)

    wg = lax.optimization_barrier(dot_tn(gpre_rel[:, :512], agg)) + got_w.astype(F32)
    up = along_y(wg[256:320].astype(BF16), 1)
    down = along_y(wg[320:384].astype(BF16), 3)
    to_up = jnp.concatenate([wg[128:192] + up.astype(F32), wg[192:256]], axis=0).astype(BF16)
    to_down = jnp.concatenate([wg[384:448], wg[448:512] + down.astype(F32)], axis=0).astype(BF16)
    wg = wg[:128] + along_y(to_up, 1).astype(F32) + along_y(to_down, 3).astype(F32)

    for bit in (4, 2, 1):
        gathered = jnp.concatenate([gathered, across_z(gathered, bit)], axis=0)
        gathered = lax.optimization_barrier(gathered)

    (to_second,) = call(
        through_kernel, [VM, VM, VM], [((both, width), BF16)], 2 * mm, roles_t, dagg, back_pair
    )
    back_second = second_step(to_second)

    sent = wg[32:].astype(BF16)
    gots = [along_x(sent[32 * (k - 1) : 32 * k], k) for k in (1, 3, 2)]
    wg = wg[:32] + (gots[0].astype(F32) + gots[1].astype(F32) + gots[2].astype(F32))

    gots = [along_x(gathered, -k) for k in (1, 3, 2)]
    (joined,) = call(
        join_kernel, [VM] * 4, [((128, 2 * width), BF16)], mm, gathered, gots[0], gots[2], gots[1]
    )
    other = swap(joined)
    for bit, rows in ((1, 16), (2, 8), (4, 4)):
        got = across_z(wg[rows:].astype(BF16), bit)
        wg = wg[:rows] + got.astype(F32)

    base, carried = call(
        base_kernel,
        [VM] * 5,
        [((both, width), F32), ((nodes, width), BF16)],
        2 * mm,
        local_t,
        dagg,
        back_pair,
        back_first,
        back_second,
    )
    (grads,) = call(
        grad_kernel, [VM] * 4, [((steps, nodes, width), BF16)], 2 * mm, base, rel_t, joined, other
    )
    scale = (both * GROUPS * XS * ZS * CORES) ** (-0.5)
    return act.reshape(steps, nodes, width), grads, carried, wg * scale


def solution(mesh):
    return jax.shard_map(
        per_device,
        mesh=mesh,
        in_specs=(
            P(None, ("group", "dom"), None),
            P(("group", "dom"), None),
            P(("group", "dom"), None),
            P(("group", "dom"), None),
            P("group", None, None, None),
            P(None, ("group", "dom")),
            P("group", "dom"),
            P(),
            P(None, ("group", "dom"), None),
        ),
        out_specs=(
            P(None, ("group", "dom"), None),
            P(None, ("group", "dom"), None),
            P(("group", "dom"), None),
            P(("group", "dom"), None),
        ),
        check_vma=False,
    )
```

```python
import jax
import jax.numpy as jnp
from jax import lax
from jax.experimental import pallas as pl
from jax.experimental.pallas import tpu as pltpu
from jax.sharding import PartitionSpec as P


BLK = 128
HUB_DEV = 4
CORES = 2
XS = 4
ZS = 8
GROUPS = 4
F32 = jnp.float32
BF16 = jnp.bfloat16


def dom_index(x, z, c):
    return (x * ZS + z) * CORES + c


def dom_pairs(target):
    pairs = []
    for x in range(XS):
        for z in range(ZS):
            for c in range(CORES):
                pairs.append((dom_index(x, z, c), target(x, z, c)))
    return pairs


def swap(v):
    return lax.ppermute(v, "dom", dom_pairs(lambda x, z, c: dom_index(x, z, 1 - c)))


def along_x(v, k):
    return lax.ppermute(v, "dom", dom_pairs(lambda x, z, c: dom_index((x + k) % XS, z, c)))


def along_z(v, k):
    return lax.ppermute(
        v, "dom", dom_pairs(lambda x, z, c: dom_index(x, (z + (k if c else -k)) % ZS, c))
    )


def along_y(v, k):
    return lax.ppermute(v, "group", [(y, (y + k) % GROUPS) for y in range(GROUPS)])


def chip_step(v, even_by):
    count = XS * ZS * CORES
    return lax.ppermute(
        v, "dom", [(d, (d + (even_by if d % 2 == 0 else -even_by)) % count) for d in range(count)]
    )


def first_step(v):
    return chip_step(v, -2)


def second_step(v):
    return chip_step(v, 2)


def offset_of(order):
    return (order // 2 + 1) * (1 - 2 * (order % 2))


def dot(a, b):
    return lax.dot_general(a, b, (((1,), (0,)), ((), ())), preferred_element_type=F32)


def dot_tn(a, b):
    return lax.dot_general(a, b, (((0,), (0,)), ((), ())), preferred_element_type=F32)


def dot_nt(a, b):
    return lax.dot_general(a, b, (((1,), (1,)), ((), ())), preferred_element_type=F32)


def relative_rows(shape, with_group, here, y):
    c = here & 1
    z = (here >> 1) & (ZS - 1)
    x = here >> 4
    r = lax.broadcasted_iota(jnp.int32, shape, 0)
    at = 4 if with_group else 2
    kz = ((r >> (at + 2)) & 1) + (((r >> (at + 1)) & 1) << 1) + (((r >> at) & 1) << 2)
    cc = c ^ (r >> (9 if with_group else 7))
    zz = (z - (2 * cc - 1) * kz) & (ZS - 1)
    low = r & 3
    if with_group:
        xx = (x + (r >> 2)) & 3
        yy = (y + (r >> 7)) & 3
        return (yy << 8) + (xx << 6) + (zz << 3) + (cc << 2) + low
    xx = (x + (r >> 5)) & 3
    return (xx << 6) + (zz << 3) + (cc << 2) + low


VM = pl.BlockSpec(memory_space=pltpu.VMEM)
SM = pl.BlockSpec(memory_space=pltpu.SMEM)
ANY = pl.BlockSpec(memory_space=pl.ANY)


def call(body, specs, outs, flops, *args):
    shapes = [jax.ShapeDtypeStruct(s, d) for s, d in outs]
    moved = sum(a.size * a.dtype.itemsize for a in args) + sum(s.size * s.dtype.itemsize for s in shapes)
    kernel = pl.pallas_call(
        body,
        out_shape=shapes,
        in_specs=specs,
        out_specs=[VM] * len(shapes),
        cost_estimate=pl.CostEstimate(flops=flops, bytes_accessed=moved, transcendentals=0),
        compiler_params=pltpu.CompilerParams(vmem_limit_bytes=16 * 1024 * 1024),
    )
    return kernel(*args)


def lane_loop(width, body):
    def step(i, carry):
        body(pl.multiple_of(i * 256, 256))
        return carry

    lax.fori_loop(0, width // 256, step, 0)


def hub_kernel(asked_ref, hub_ref, f_ref, rel_ref, pay_ref, f0_ref, mine_ref):
    target = relative_rows((256, 256), False, lax.axis_index("dom"), 0)
    col = lax.broadcasted_iota(jnp.int32, (256, 256), 1)
    perm = jnp.where(target == col, 1.0, 0.0).astype(BF16)
    ordered = dot(perm, hub_ref[...])
    rel = ordered.astype(BF16)
    rel_ref[...] = jnp.transpose(ordered).astype(BF16)

    def some(n):
        lanes = pl.ds(n, 256)
        for t in range(2):
            p = dot(rel, f_ref[t, :, lanes])
            mine_ref[:, pl.ds(t * 1024 + n, 256)] = p[:128]
            pay_ref[t * 128 : t * 128 + 128, lanes] = p[128:].astype(BF16)
        pay_ref[256:512, lanes] = f_ref[0, :, lanes]
        f0_ref[:, lanes] = f_ref[0, :, lanes]

    lane_loop(1024, some)


def perm_kernel(out_ref):
    target = relative_rows((1024, 128), True, lax.axis_index("dom"), lax.axis_index("group"))
    col = lax.broadcasted_iota(jnp.int32, (1024, 128), 1)
    off = target - col
    for n in range(8):
        out_ref[:, n * 128 : n * 128 + 128] = jnp.where(off == n * 128, 1.0, 0.0).astype(BF16)


def table_kernel(present, asked_ref, b_ref, a_ref, roles_ref, roles_t_ref, local_ref, local_t_ref):
    here = lax.axis_index("dom")
    c = here & 1
    asked = asked_ref[0, here]
    for r in range(4):
        for b in range(2):
            total = None
            for o in (r, r ^ 1):
                source = here + offset_of(o)
                inside = ((r ^ c) == o) & (source >= 0) & (source < XS * ZS * CORES)
                for j in range(2):
                    s = 2 * o + j
                    gate = jnp.where(inside & (asked[o : o + 1, j : j + 1] == b), 1.0, 0.0)
                    term = b_ref[:, s * BLK : s * BLK + BLK].astype(F32) * gate
                    total = term if total is None else total + term
            at = (2 * r + b) * BLK
            roles_ref[:, at : at + BLK] = total.astype(BF16)
            roles_t_ref[at : at + BLK, :] = jnp.transpose(total).astype(BF16)
    for i in range(2):
        for j in range(2):
            gate = present[i, j].astype(F32)
            tile = a_ref[i * BLK : i * BLK + BLK, j * BLK : j * BLK + BLK].astype(F32) * gate
            local_ref[i * BLK : i * BLK + BLK, j * BLK : j * BLK + BLK] = tile.astype(BF16)
            local_t_ref[j * BLK : j * BLK + BLK, i * BLK : i * BLK + BLK] = jnp.transpose(tile).astype(BF16)


def open_kernel(got_ref, mine_ref, keep_ref, *send_refs):
    def some(n):
        for t in range(2):
            lanes = pl.ds(t * 1024 + n, 256)
            part = mine_ref[:, lanes] + got_ref[t * 128 : t * 128 + 128, pl.ds(n, 256)].astype(F32)
            keep_ref[:, lanes] = part[:32]
            for k in range(3):
                send_refs[k][:, lanes] = part[32 * k + 32 : 32 * k + 64].astype(BF16)

    lane_loop(1024, some)


def total_kernel(after, roles, local, f_ref, pair_ref, far_ref, first_ref, out_ref):
    def some(n):
        lanes = pl.ds(n, 256)
        bound = (
            dot(roles[:, :256], pair_ref[256:512, lanes])
            + dot(roles[:, 256:512], far_ref[:, lanes])
            + dot(roles[:, 512:768], first_ref[:, lanes])
        )
        for t in range(2):
            out_ref[t * 256 : t * 256 + 256, lanes] = bound + dot(local[...], f_ref[t, :, lanes])

    lane_loop(1024, some)


def agg_kernel(offs, roles, second_ref, total_ref, own_ref, g1_ref, g2_ref, g3_ref, agg_ref):
    ids = lax.broadcasted_iota(jnp.int32, (64, 256), 0)

    def some(n):
        lanes = pl.ds(n, 256)
        bound = dot(roles[:, 768:], second_ref[:, lanes])
        for t in range(2):
            at_t = pl.ds(t * 1024 + n, 256)
            hubs = own_ref[:, at_t] + (
                g1_ref[:, at_t].astype(F32) + g2_ref[:, at_t].astype(F32) + g3_ref[:, at_t].astype(F32)
            )
            for i in range(HUB_DEV):
                at = t * 256 + i * 64
                extra = jnp.where(ids == offs[0, i], hubs[i : i + 1], 0.0)
                rest = total_ref[at : at + 64, lanes] + bound[i * 64 : i * 64 + 64]
                agg_ref[at : at + 64, lanes] = (rest + extra).astype(BF16)

    lane_loop(1024, some)


def send_kernel(offs, roles_t, dagg_ref, mirror_ref, *first_refs):
    cols = lax.broadcasted_iota(jnp.int32, (8, 256), 1)
    rows = lax.broadcasted_iota(jnp.int32, (8, 256), 0)
    where = jnp.where(
        rows == 0, offs[0, 0], jnp.where(rows == 1, offs[0, 1], jnp.where(rows == 2, offs[0, 2], offs[0, 3]))
    )
    pick = jnp.where((cols == rows * 64 + where) & (rows < HUB_DEV), 1.0, 0.0).astype(BF16)

    def some(n):
        lanes = pl.ds(n, 256)
        for t in range(2):
            d = dagg_ref[t * 256 : t * 256 + 256, lanes]
            mirror_ref[:, pl.ds(t * 1024 + n, 256)] = dot(pick, d)[:HUB_DEV].astype(BF16)
            first_refs[t][:, lanes] = dot(roles_t[768:, :], d).astype(BF16)

    lane_loop(1024, some)


def role_kernel(r, roles_t, dagg_ref, out_ref):
    def some(n):
        lanes = pl.ds(n, 256)
        for t in range(2):
            rows = slice(t * 256, t * 256 + 256)
            out_ref[rows, lanes] = dot(roles_t[r * 256 : r * 256 + 256, :], dagg_ref[rows, lanes]).astype(BF16)

    lane_loop(1024, some)


def near_kernel(*refs):
    role_kernel(0, *refs)


def far_kernel(*refs):
    role_kernel(1, *refs)


def through_kernel(roles_t, dagg_ref, got_ref, out_ref):
    def some(n):
        lanes = pl.ds(n, 256)
        for t in range(2):
            rows = slice(t * 256, t * 256 + 256)
            mine = dot(roles_t[512:768, :], dagg_ref[rows, lanes])
            out_ref[rows, lanes] = (mine + got_ref[rows, lanes].astype(F32)).astype(BF16)

    lane_loop(1024, some)


def base_kernel(local_t, dagg_ref, pair_ref, first0_ref, first1_ref, second_ref, base_ref, carried_ref):
    def some(n):
        lanes = pl.ds(n, 256)
        firsts = (first0_ref, first1_ref)
        local = [dot(local_t[...], dagg_ref[t * 256 : t * 256 + 256, lanes]) for t in range(2)]
        back = [
            pair_ref[t * 256 : t * 256 + 256, lanes].astype(F32)
            + firsts[t][:, lanes].astype(F32)
            + second_ref[t * 256 : t * 256 + 256, lanes].astype(F32)
            for t in range(2)
        ]
        base_ref[:256, lanes] = local[0]
        base_ref[256:, lanes] = local[1] + back[0]
        carried_ref[:, lanes] = back[1].astype(BF16)

    lane_loop(1024, some)


def grad_kernel(base_ref, rel_t, own_ref, got_ref, out_ref):
    def some(n):
        for t in range(2):
            lanes = pl.ds(t * 1024 + n, 256)
            hub = dot(rel_t[:, :128], own_ref[:, lanes]) + dot(rel_t[:, 128:], got_ref[:, lanes])
            out_ref[t, :, pl.ds(n, 256)] = (base_ref[t * 256 : t * 256 + 256, pl.ds(n, 256)] + hub).astype(BF16)

    lane_loop(1024, some)


def join_kernel(own_ref, one_ref, two_ref, three_ref, out_ref):
    out_ref[:32, :] = own_ref[...]
    out_ref[32:64, :] = one_ref[...]
    out_ref[64:96, :] = two_ref[...]
    out_ref[96:, :] = three_ref[...]


def per_device(
    features,
    adjacency,
    tile_mask,
    boundary_adj,
    boundary_blocks,
    hub_adj,
    hub_offsets,
    weight,
    cotangent,
):
    steps, nodes, width = features.shape
    both = steps * nodes
    mm = 2 * nodes * nodes * width

    rel_t, payload, first, mine = call(
        hub_kernel,
        [VM, VM, VM],
        [((256, 256), BF16), ((512, width), BF16), ((nodes, width), BF16), ((128, 2 * width), F32)],
        2 * mm,
        boundary_blocks,
        hub_adj,
        features,
    )
    from_pair = swap(payload)
    from_first = first_step(first)
    from_second = second_step(first)

    roles, roles_t, local, local_t = call(
        table_kernel,
        [SM, VM, VM, VM],
        [((nodes, width), BF16), ((width, nodes), BF16), ((nodes, nodes), BF16), ((nodes, nodes), BF16)],
        mm,
        tile_mask,
        boundary_blocks,
        boundary_adj,
        adjacency,
    )

    (perm,) = call(perm_kernel, [], [((width, width), BF16)], mm)
    part, *sends = call(
        open_kernel,
        [VM, VM],
        [((32, 2 * width), F32)] + [((32, 2 * width), BF16)] * 3,
        mm,
        from_pair,
        mine,
    )
    gots = [along_x(sends[k - 1], k) for k in (1, 3, 2)]
    from_far = swap(from_first)
    part = part + (gots[0].astype(F32) + gots[1].astype(F32) + gots[2].astype(F32))
    marks = []
    for k, rows in ((1, 16), (2, 8), (4, 4)):
        sent = part[rows:].astype(BF16)
        marks.append(sent)
        got = along_z(sent, -k)
        part = part[:rows] + got.astype(F32)
    sent = part.astype(BF16)
    gots = [along_y(sent, k) for k in (1, 3, 2)]

    (total,) = call(
        total_kernel,
        [ANY, VM, VM, VM, VM, VM, VM],
        [((both, width), F32)],
        6 * mm,
        marks[1],
        roles,
        local,
        features,
        from_pair,
        from_far,
        from_first,
    )
    (agg,) = call(
        agg_kernel,
        [SM, VM, VM, VM, VM, VM, VM, VM],
        [((both, width), BF16)],
        mm,
        hub_offsets,
        roles,
        from_second,
        total,
        part,
        *gots,
    )
    pre = dot_nt(agg, weight)
    sig = jax.nn.sigmoid(pre)
    act = (pre * sig).astype(BF16)
    gpre = (cotangent.reshape(both, width).astype(F32) * sig * (1.0 + pre * (1.0 - sig))).astype(BF16)

    gpre_rel = lax.optimization_barrier(dot_nt(gpre, perm).astype(BF16))
    got_w = swap(dot_tn(gpre_rel[:, 512:], agg).astype(BF16))
    dagg = dot(gpre, weight).astype(BF16)

    (to_far,) = call(far_kernel, [VM, VM], [((both, width), BF16)], 2 * mm, roles_t, dagg)
    got_far = swap(to_far)
    mirror, *to_first = call(
        send_kernel,
        [SM, VM, VM],
        [((HUB_DEV, 2 * width), BF16)] + [((nodes, width), BF16)] * 2,
        2 * mm,
        hub_offsets,
        roles_t,
        dagg,
    )
    gots = [along_y(mirror, k) for k in (1, 3, 2)]
    (to_second,) = call(
        through_kernel, [VM, VM, VM], [((both, width), BF16)], 2 * mm, roles_t, dagg, got_far
    )
    back_second = second_step(to_second)
    back_first = [first_step(to_first[t]) for t in range(2)]
    (to_near,) = call(near_kernel, [VM, VM], [((both, width), BF16)], 2 * mm, roles_t, dagg)
    back_pair = swap(to_near)
    gathered = (
        mirror.astype(F32) + (gots[0].astype(F32) + gots[1].astype(F32) + gots[2].astype(F32))
    ).astype(BF16)

    wg = lax.optimization_barrier(dot_tn(gpre_rel[:, :512], agg)) + got_w.astype(F32)
    up = along_y(wg[256:320].astype(BF16), 1)
    down = along_y(wg[320:384].astype(BF16), 3)
    to_up = jnp.concatenate([wg[128:192] + up.astype(F32), wg[192:256]], axis=0).astype(BF16)
    to_down = jnp.concatenate([wg[384:448], wg[448:512] + down.astype(F32)], axis=0).astype(BF16)
    wg = wg[:128] + along_y(to_up, 1).astype(F32) + along_y(to_down, 3).astype(F32)
    for k, rows in ((1, 64), (2, 32), (4, 16)):
        got = along_z(wg[rows:].astype(BF16), -k)
        wg = wg[:rows] + got.astype(F32)
    sent = wg.astype(BF16)
    gots = [along_x(sent[4 * k : 4 * k + 4], k) for k in (1, 3, 2)]
    wg = wg[:4] + (gots[0].astype(F32) + gots[1].astype(F32) + gots[2].astype(F32))

    for k in (4, 2, 1):
        gathered = jnp.concatenate([gathered, along_z(gathered, k)], axis=0)
        gathered = lax.optimization_barrier(gathered)
    gots = [along_x(gathered, -k) for k in (1, 3, 2)]
    (joined,) = call(
        join_kernel, [VM] * 4, [((128, 2 * width), BF16)], mm, gathered, gots[0], gots[2], gots[1]
    )
    other = swap(joined)

    base, carried = call(
        base_kernel,
        [VM] * 6,
        [((both, width), F32), ((nodes, width), BF16)],
        2 * mm,
        local_t,
        dagg,
        back_pair,
        *back_first,
        back_second,
    )
    (grads,) = call(
        grad_kernel, [VM] * 4, [((steps, nodes, width), BF16)], 2 * mm, base, rel_t, joined, other
    )
    scale = (both * GROUPS * XS * ZS * CORES) ** (-0.5)
    return act.reshape(steps, nodes, width), grads, carried, wg * scale


def solution(mesh):
    return jax.shard_map(
        per_device,
        mesh=mesh,
        in_specs=(
            P(None, ("group", "dom"), None),
            P(("group", "dom"), None),
            P(("group", "dom"), None),
            P(("group", "dom"), None),
            P("group", None, None, None),
            P(None, ("group", "dom")),
            P("group", "dom"),
            P(),
            P(None, ("group", "dom"), None),
        ),
        out_specs=(
            P(None, ("group", "dom"), None),
            P(None, ("group", "dom"), None),
            P(("group", "dom"), None),
            P(("group", "dom"), None),
        ),
        check_vma=False,
    )
```

```python
import jax
import jax.numpy as jnp
from jax import lax
from jax.experimental import pallas as pl
from jax.experimental.pallas import tpu as pltpu
from jax.sharding import PartitionSpec as P


BLK = 128
HUB_DEV = 4
CORES = 2
XS = 4
ZS = 8
GROUPS = 4
F32 = jnp.float32
BF16 = jnp.bfloat16


def dom_index(x, z, c):
    return (x * ZS + z) * CORES + c


def dom_pairs(target):
    pairs = []
    for x in range(XS):
        for z in range(ZS):
            for c in range(CORES):
                pairs.append((dom_index(x, z, c), target(x, z, c)))
    return pairs


def swap(v):
    return lax.ppermute(v, "dom", dom_pairs(lambda x, z, c: dom_index(x, z, 1 - c)))


def along_x(v, k):
    return lax.ppermute(v, "dom", dom_pairs(lambda x, z, c: dom_index((x + k) % XS, z, c)))


def along_z(v, k):
    return lax.ppermute(
        v, "dom", dom_pairs(lambda x, z, c: dom_index(x, (z + (k if c else -k)) % ZS, c))
    )


def along_y(v, k):
    return lax.ppermute(v, "group", [(y, (y + k) % GROUPS) for y in range(GROUPS)])


def chip_step(v, even_by):
    count = XS * ZS * CORES
    return lax.ppermute(
        v, "dom", [(d, (d + (even_by if d % 2 == 0 else -even_by)) % count) for d in range(count)]
    )


def first_step(v):
    return chip_step(v, -2)


def second_step(v):
    return chip_step(v, 2)


def offset_of(order):
    return (order // 2 + 1) * (1 - 2 * (order % 2))


def dot(a, b):
    return lax.dot_general(a, b, (((1,), (0,)), ((), ())), preferred_element_type=F32)


def dot_tn(a, b):
    return lax.dot_general(a, b, (((0,), (0,)), ((), ())), preferred_element_type=F32)


def dot_nt(a, b):
    return lax.dot_general(a, b, (((1,), (1,)), ((), ())), preferred_element_type=F32)


def relative_rows(shape, with_group, here, y):
    c = here & 1
    z = (here >> 1) & (ZS - 1)
    x = here >> 4
    r = lax.broadcasted_iota(jnp.int32, shape, 0)
    at = 4 if with_group else 2
    kz = ((r >> (at + 2)) & 1) + (((r >> (at + 1)) & 1) << 1) + (((r >> at) & 1) << 2)
    cc = c ^ (r >> (9 if with_group else 7))
    zz = (z - (2 * cc - 1) * kz) & (ZS - 1)
    low = r & 3
    if with_group:
        xx = (x + (r >> 2)) & 3
        yy = (y + (r >> 7)) & 3
        return (yy << 8) + (xx << 6) + (zz << 3) + (cc << 2) + low
    xx = (x + (r >> 5)) & 3
    return (xx << 6) + (zz << 3) + (cc << 2) + low


VM = pl.BlockSpec(memory_space=pltpu.VMEM)
SM = pl.BlockSpec(memory_space=pltpu.SMEM)
ANY = pl.BlockSpec(memory_space=pl.ANY)


def call(body, specs, outs, flops, *args):
    shapes = [jax.ShapeDtypeStruct(s, d) for s, d in outs]
    moved = sum(a.size * a.dtype.itemsize for a in args) + sum(s.size * s.dtype.itemsize for s in shapes)
    kernel = pl.pallas_call(
        body,
        out_shape=shapes,
        in_specs=specs,
        out_specs=[VM] * len(shapes),
        cost_estimate=pl.CostEstimate(flops=flops, bytes_accessed=moved, transcendentals=0),
        compiler_params=pltpu.CompilerParams(vmem_limit_bytes=16 * 1024 * 1024),
    )
    return kernel(*args)


def lane_loop(width, body, together=1):
    def step(i, carry):
        for j in range(together):
            body(pl.multiple_of(i * (256 * together) + j * 256, 256))
        return carry

    lax.fori_loop(0, width // (256 * together), step, 0)


def hub_kernel(asked_ref, hub_ref, f_ref, rel_ref, pay_ref, f0_ref, mine_ref):
    target = relative_rows((256, 256), False, lax.axis_index("dom"), 0)
    col = lax.broadcasted_iota(jnp.int32, (256, 256), 1)
    perm = jnp.where(target == col, 1.0, 0.0).astype(BF16)
    ordered = dot(perm, hub_ref[...])
    rel = ordered.astype(BF16)
    rel_ref[...] = jnp.transpose(ordered).astype(BF16)

    def some(n):
        lanes = pl.ds(n, 256)
        for t in range(2):
            p = dot(rel, f_ref[t, :, lanes])
            mine_ref[:, pl.ds(t * 1024 + n, 256)] = p[:128]
            pay_ref[t * 128 : t * 128 + 128, lanes] = p[128:].astype(BF16)
        pay_ref[256:512, lanes] = f_ref[0, :, lanes]
        f0_ref[:, lanes] = f_ref[0, :, lanes]

    lane_loop(1024, some)


def perm_kernel(out_ref):
    target = relative_rows((1024, 128), True, lax.axis_index("dom"), lax.axis_index("group"))
    off = target - lax.broadcasted_iota(jnp.int32, (1024, 128), 1)

    def some(i, carry):
        at = pl.multiple_of(i * 128, 128)
        out_ref[:, pl.ds(at, 128)] = jnp.where(off == at, 1.0, 0.0).astype(BF16)
        return carry

    lax.fori_loop(0, 8, some, 0)


def table_kernel(
    present, asked_ref, b_ref, a_ref, roles_ref, roles_t_ref, local_ref, local_t_ref
):
    here = lax.axis_index("dom")
    c = here & 1
    asked = asked_ref[0, here]

    def some(i, carry):
        rows = pl.ds(pl.multiple_of(i * BLK, BLK), BLK)
        for r in range(4):
            for b in range(2):
                total = None
                for o in (r, r ^ 1):
                    source = here + offset_of(o)
                    inside = ((r ^ c) == o) & (source >= 0) & (source < XS * ZS * CORES)
                    for j in range(2):
                        s = 2 * o + j
                        gate = jnp.where(inside & (asked[o : o + 1, j : j + 1] == b), 1.0, 0.0)
                        term = b_ref[rows, s * BLK : s * BLK + BLK].astype(F32) * gate
                        total = term if total is None else total + term
                at = (2 * r + b) * BLK
                roles_ref[rows, at : at + BLK] = total.astype(BF16)
                roles_t_ref[at : at + BLK, rows] = jnp.transpose(total).astype(BF16)
        for j in range(2):
            gate = present[i, j].astype(F32)
            tile = a_ref[rows, j * BLK : j * BLK + BLK].astype(F32) * gate
            local_ref[rows, j * BLK : j * BLK + BLK] = tile.astype(BF16)
            local_t_ref[j * BLK : j * BLK + BLK, rows] = jnp.transpose(tile).astype(BF16)
        return carry

    lax.fori_loop(0, 2, some, 0)


def open_kernel(got_ref, mine_ref, keep_ref, *send_refs):
    def some(n):
        for t in range(2):
            lanes = pl.ds(t * 1024 + n, 256)
            part = mine_ref[:, lanes] + got_ref[t * 128 : t * 128 + 128, pl.ds(n, 256)].astype(F32)
            keep_ref[:, lanes] = part[:32]
            for k in range(3):
                send_refs[k][:, lanes] = part[32 * k + 32 : 32 * k + 64].astype(BF16)

    lane_loop(1024, some)


def total_kernel(after, roles, local, f_ref, pair_ref, far_ref, first_ref, out_ref):
    def some(n):
        lanes = pl.ds(n, 256)
        bound = (
            dot(roles[:, :256], pair_ref[256:512, lanes])
            + dot(roles[:, 256:512], far_ref[:, lanes])
            + dot(roles[:, 512:768], first_ref[:, lanes])
        )
        for t in range(2):
            out_ref[t * 256 : t * 256 + 256, lanes] = bound + dot(local[...], f_ref[t, :, lanes])

    lane_loop(1024, some)


def agg_kernel(offs, roles, second_ref, total_ref, own_ref, g1_ref, g2_ref, g3_ref, agg_ref):
    ids = lax.broadcasted_iota(jnp.int32, (64, 256), 0)

    def some(n):
        lanes = pl.ds(n, 256)
        bound = dot(roles[:, 768:], second_ref[:, lanes])
        for t in range(2):
            at_t = pl.ds(t * 1024 + n, 256)
            hubs = own_ref[:, at_t] + (
                g1_ref[:, at_t].astype(F32) + g2_ref[:, at_t].astype(F32) + g3_ref[:, at_t].astype(F32)
            )
            for i in range(HUB_DEV):
                at = t * 256 + i * 64
                extra = jnp.where(ids == offs[0, i], hubs[i : i + 1], 0.0)
                rest = total_ref[at : at + 64, lanes] + bound[i * 64 : i * 64 + 64]
                agg_ref[at : at + 64, lanes] = (rest + extra).astype(BF16)

    lane_loop(1024, some)


def send_kernel(offs, roles_t, dagg_ref, mirror_ref, *first_refs):
    cols = lax.broadcasted_iota(jnp.int32, (8, 256), 1)
    rows = lax.broadcasted_iota(jnp.int32, (8, 256), 0)
    where = jnp.where(
        rows == 0, offs[0, 0], jnp.where(rows == 1, offs[0, 1], jnp.where(rows == 2, offs[0, 2], offs[0, 3]))
    )
    pick = jnp.where((cols == rows * 64 + where) & (rows < HUB_DEV), 1.0, 0.0).astype(BF16)

    def some(n):
        lanes = pl.ds(n, 256)
        for t in range(2):
            d = dagg_ref[t * 256 : t * 256 + 256, lanes]
            mirror_ref[:, pl.ds(t * 1024 + n, 256)] = dot(pick, d)[:HUB_DEV].astype(BF16)
            first_refs[t][:, lanes] = dot(roles_t[768:, :], d).astype(BF16)

    lane_loop(1024, some)


def role_kernel(r, roles_t, dagg_ref, out_ref):
    def some(n):
        lanes = pl.ds(n, 256)
        for t in range(2):
            rows = slice(t * 256, t * 256 + 256)
            out_ref[rows, lanes] = dot(roles_t[r * 256 : r * 256 + 256, :], dagg_ref[rows, lanes]).astype(BF16)

    lane_loop(1024, some, 2)


def near_kernel(*refs):
    role_kernel(0, *refs)


def far_kernel(*refs):
    role_kernel(1, *refs)


def through_kernel(roles_t, dagg_ref, got_ref, out_ref):
    def some(n):
        lanes = pl.ds(n, 256)
        for t in range(2):
            rows = slice(t * 256, t * 256 + 256)
            mine = dot(roles_t[512:768, :], dagg_ref[rows, lanes])
            out_ref[rows, lanes] = (mine + got_ref[rows, lanes].astype(F32)).astype(BF16)

    lane_loop(1024, some)


def base_kernel(local_t, dagg_ref, pair_ref, first0_ref, first1_ref, second_ref, base_ref, carried_ref):
    def some(n):
        lanes = pl.ds(n, 256)
        firsts = (first0_ref, first1_ref)
        local = [dot(local_t[...], dagg_ref[t * 256 : t * 256 + 256, lanes]) for t in range(2)]
        back = [
            pair_ref[t * 256 : t * 256 + 256, lanes].astype(F32)
            + firsts[t][:, lanes].astype(F32)
            + second_ref[t * 256 : t * 256 + 256, lanes].astype(F32)
            for t in range(2)
        ]
        base_ref[:256, lanes] = local[0]
        base_ref[256:, lanes] = local[1] + back[0]
        carried_ref[:, lanes] = back[1].astype(BF16)

    lane_loop(1024, some)


def grad_kernel(base_ref, rel_t, own_ref, got_ref, out_ref):
    def some(n):
        for t in range(2):
            lanes = pl.ds(t * 1024 + n, 256)
            hub = dot(rel_t[:, :128], own_ref[:, lanes]) + dot(rel_t[:, 128:], got_ref[:, lanes])
            out_ref[t, :, pl.ds(n, 256)] = (base_ref[t * 256 : t * 256 + 256, pl.ds(n, 256)] + hub).astype(BF16)

    lane_loop(1024, some, 2)


def join_kernel(own_ref, one_ref, two_ref, three_ref, out_ref):
    out_ref[:32, :] = own_ref[...]
    out_ref[32:64, :] = one_ref[...]
    out_ref[64:96, :] = two_ref[...]
    out_ref[96:, :] = three_ref[...]


def per_device(
    features,
    adjacency,
    tile_mask,
    boundary_adj,
    boundary_blocks,
    hub_adj,
    hub_offsets,
    weight,
    cotangent,
):
    steps, nodes, width = features.shape
    both = steps * nodes
    mm = 2 * nodes * nodes * width

    rel_t, payload, first, mine = call(
        hub_kernel,
        [VM, VM, VM],
        [((256, 256), BF16), ((512, width), BF16), ((nodes, width), BF16), ((128, 2 * width), F32)],
        2 * mm,
        boundary_blocks,
        hub_adj,
        features,
    )
    from_pair = swap(payload)
    from_first = first_step(first)
    from_second = second_step(first)

    roles, roles_t, local, local_t = call(
        table_kernel,
        [SM, VM, VM, VM],
        [((nodes, width), BF16), ((width, nodes), BF16), ((nodes, nodes), BF16), ((nodes, nodes), BF16)],
        mm,
        tile_mask,
        boundary_blocks,
        boundary_adj,
        adjacency,
    )

    (perm,) = call(perm_kernel, [], [((width, width), BF16)], mm)
    part, *sends = call(
        open_kernel,
        [VM, VM],
        [((32, 2 * width), F32)] + [((32, 2 * width), BF16)] * 3,
        mm,
        from_pair,
        mine,
    )
    gots = [along_x(sends[k - 1], k) for k in (1, 3, 2)]
    from_far = swap(from_first)
    part = part + (gots[0].astype(F32) + gots[1].astype(F32) + gots[2].astype(F32))
    marks = []
    for k, rows in ((1, 16), (2, 8), (4, 4)):
        sent = part[rows:].astype(BF16)
        marks.append(sent)
        got = along_z(sent, -k)
        part = part[:rows] + got.astype(F32)
    sent = part.astype(BF16)
    gots = [along_y(sent, k) for k in (1, 3, 2)]

    (total,) = call(
        total_kernel,
        [ANY, VM, VM, VM, VM, VM, VM],
        [((both, width), F32)],
        6 * mm,
        marks[1],
        roles,
        local,
        features,
        from_pair,
        from_far,
        from_first,
    )
    (agg,) = call(
        agg_kernel,
        [SM, VM, VM, VM, VM, VM, VM, VM],
        [((both, width), BF16)],
        mm,
        hub_offsets,
        roles,
        from_second,
        total,
        part,
        *gots,
    )
    pre = dot_nt(agg, weight)
    sig = jax.nn.sigmoid(pre)
    act = (pre * sig).astype(BF16)
    gpre = (cotangent.reshape(both, width).astype(F32) * sig * (1.0 + pre * (1.0 - sig))).astype(BF16)

    gpre_rel = lax.optimization_barrier(dot_nt(gpre, perm).astype(BF16))
    got_w = swap(dot_tn(gpre_rel[:, 512:], agg).astype(BF16))
    dagg = dot(gpre, weight).astype(BF16)

    (to_far,) = call(far_kernel, [VM, VM], [((both, width), BF16)], 2 * mm, roles_t, dagg)
    got_far = swap(to_far)
    mirror, *to_first = call(
        send_kernel,
        [SM, VM, VM],
        [((HUB_DEV, 2 * width), BF16)] + [((nodes, width), BF16)] * 2,
        2 * mm,
        hub_offsets,
        roles_t,
        dagg,
    )
    gots = [along_y(mirror, k) for k in (1, 3, 2)]
    (to_second,) = call(
        through_kernel, [VM, VM, VM], [((both, width), BF16)], 2 * mm, roles_t, dagg, got_far
    )
    back_second = second_step(to_second)
    back_first = [first_step(to_first[t]) for t in range(2)]
    (to_near,) = call(near_kernel, [VM, VM], [((both, width), BF16)], 2 * mm, roles_t, dagg)
    back_pair = swap(to_near)
    gathered = (
        mirror.astype(F32) + (gots[0].astype(F32) + gots[1].astype(F32) + gots[2].astype(F32))
    ).astype(BF16)

    wg = lax.optimization_barrier(dot_tn(gpre_rel[:, :512], agg)) + got_w.astype(F32)
    up = along_y(wg[256:320].astype(BF16), 1)
    down = along_y(wg[320:384].astype(BF16), 3)
    to_up = jnp.concatenate([wg[128:192] + up.astype(F32), wg[192:256]], axis=0).astype(BF16)
    to_down = jnp.concatenate([wg[384:448], wg[448:512] + down.astype(F32)], axis=0).astype(BF16)
    wg = wg[:128] + along_y(to_up, 1).astype(F32) + along_y(to_down, 3).astype(F32)
    for k, rows in ((1, 64), (2, 32), (4, 16)):
        got = along_z(wg[rows:].astype(BF16), -k)
        wg = wg[:rows] + got.astype(F32)
    sent = wg.astype(BF16)
    gots = [along_x(sent[4 * k : 4 * k + 4], k) for k in (1, 3, 2)]
    wg = wg[:4] + (gots[0].astype(F32) + gots[1].astype(F32) + gots[2].astype(F32))

    for k in (4, 2, 1):
        gathered = jnp.concatenate([gathered, along_z(gathered, k)], axis=0)
        gathered = lax.optimization_barrier(gathered)
    gots = [along_x(gathered, -k) for k in (1, 3, 2)]
    (joined,) = call(
        join_kernel, [VM] * 4, [((128, 2 * width), BF16)], mm, gathered, gots[0], gots[2], gots[1]
    )
    other = swap(joined)

    base, carried = call(
        base_kernel,
        [VM] * 6,
        [((both, width), F32), ((nodes, width), BF16)],
        2 * mm,
        local_t,
        dagg,
        back_pair,
        *back_first,
        back_second,
    )
    (grads,) = call(
        grad_kernel, [VM] * 4, [((steps, nodes, width), BF16)], 2 * mm, base, rel_t, joined, other
    )
    scale = (both * GROUPS * XS * ZS * CORES) ** (-0.5)
    return act.reshape(steps, nodes, width), grads, carried, wg * scale


def solution(mesh):
    return jax.shard_map(
        per_device,
        mesh=mesh,
        in_specs=(
            P(None, ("group", "dom"), None),
            P(("group", "dom"), None),
            P(("group", "dom"), None),
            P(("group", "dom"), None),
            P("group", None, None, None),
            P(None, ("group", "dom")),
            P("group", "dom"),
            P(),
            P(None, ("group", "dom"), None),
        ),
        out_specs=(
            P(None, ("group", "dom"), None),
            P(None, ("group", "dom"), None),
            P(("group", "dom"), None),
            P(("group", "dom"), None),
        ),
        check_vma=False,
    )
```
